32 devices in a mesh: lon: 4 (over y, core), lat: 8 (over z, x).
Axes of the slice: x: 2, y: 2, z: 4, core: 2. Of those that a mesh axis runs over, the one named last changes fastest.
Arguments:
- fields: bfloat16 [20, 16, 1024, 512], P(None, None, 'lat', 'lon'), may hold values from -16 to 16
- area: float32 [1024, 512], P('lat', 'lon'), may hold values from 0.2 to 5
- ocean: int32 [16, 1024, 512], P(None, 'lat', 'lon'), may hold values 0 or 1
- partner: int32 [512], replicated, may hold values from 0 to 511, as said below
- counted: int32 [512], replicated, may hold values from 0 to 1, as said below
Outputs:
- zonal_mean: float32 [20, 16, 1024], replicated
The draws below stay inside these ranges and needn't reach their ends.
Inputs may be any that keep to these rules, and one draw needn't show every extreme that they name: partner pairs the columns: partner[partner[i]] = i and partner[i] != i. Of each pair i, partner[i] exactly one has counted = 1.
All inputs are finite; a program needn't handle non-finite values. No bound on the sum of `ocean` on one device may be relied on, other than what follows from the above.
Results may differ from the reference program's by a relative error of at most 0.0003.
Values may be sent and summed in bfloat16 or wider, within the bound.
A program may use at most 64 MiB of HBM per device.

```python
import math
import jax
import jax.numpy as jnp
from jax import lax

F = 20
LEV = 16
NLAT = 1024
NLON = 512


def fold_pairs(key):
    shuffled = jax.random.permutation(jax.random.fold_in(key, 7), NLON).astype(jnp.int32)
    firsts = shuffled[0::2]
    seconds = shuffled[1::2]
    partner = jnp.zeros((NLON,), jnp.int32).at[firsts].set(seconds).at[seconds].set(firsts)
    choose = jax.random.randint(jax.random.fold_in(key, 11), (NLON // 2,), 0, 2).astype(jnp.int32)
    counted = jnp.zeros((NLON,), jnp.int32).at[firsts].set(choose).at[seconds].set(1 - choose)
    return (partner, counted)


def draw_partner(key, part):
    return fold_pairs(key)[0]


def draw_counted(key, part):
    return fold_pairs(key)[1]


def draw_fields(key, part):
    key_offset = jax.random.fold_in(key, 1)
    key_noise = jax.random.fold_in(key, 2)
    offset = jax.random.normal(key_offset, (F, LEV, NLAT, 1), jnp.float32)
    spread = 1.5
    noise = jax.random.normal(key_noise, (F, LEV, NLAT, NLON), jnp.float32)
    return jnp.clip(offset + spread * noise, -16.0, 16.0).astype(jnp.bfloat16)


def set_ends(entries, stream_key, smallest, high):
    index_at = [jax.random.randint(jax.random.fold_in(stream_key, axis), (), 0, length) for axis, length in enumerate(entries.shape)]
    widest = entries.shape.index(max(entries.shape))
    beside = index_at[:widest] + [(index_at[widest] + 1) % entries.shape[widest]] + index_at[widest + 1:]
    return entries.at[tuple(index_at)].set(smallest).at[tuple(beside)].set(high)


def steps_of(key, shape, cuts, smallest, top_value):
    factor_of, own = 1.0, jax.random.fold_in(key, 6)
    for position, parts in cuts:
        draws = jnp.exp(jax.random.uniform(jax.random.fold_in(own, position), (parts,), jnp.float32, smallest / len(cuts), top_value / len(cuts)))
        factor_of = factor_of * jnp.repeat(draws, shape[position] // parts).reshape([-1 if axis == position else 1 for axis in range(len(shape))])
    return factor_of


def setup_inputs(seed: int = 0) -> dict:
    streams_of = jax.random.split(jax.random.key(seed), 6)
    fields = draw_fields(jax.random.fold_in(streams_of[5], 71), 0)
    area = jnp.clip(jnp.exp(math.log(5.0) - 3.218876 * jax.random.uniform(streams_of[1], (NLAT, NLON), jnp.float32) ** steps_of(streams_of[1], (NLAT, NLON), ((0, 8), (1, 4)), -0.2, 0.2)), 0.2, 5.0)
    ocean = set_ends((jax.random.randint(streams_of[2], (LEV, NLAT, NLON), 0, 4) < 3).astype(jnp.int32), jax.random.fold_in(streams_of[2], 1), 0, 1)
    partner = draw_partner(jax.random.fold_in(streams_of[5], 71), 0)
    counted = draw_counted(jax.random.fold_in(streams_of[5], 71), 0)
    return dict(fields=fields, area=area, ocean=ocean, partner=partner, counted=counted)


def reference(fields, area, ocean, partner, counted):
    row_index = jnp.arange(NLAT)[:, None]
    counted_weight = jnp.where(row_index == NLAT - 1, counted.astype(jnp.float32)[None, :], jnp.float32(1.0))
    cell_weight = counted_weight * area
    oceanic = ocean.astype(jnp.float32)
    weight = cell_weight[None] * oceanic
    row_weight = jnp.sum(cell_weight[None] * (oceanic + 0.05), axis=-1)
    fold_values = fields[:, :, NLAT - 1, :].astype(jnp.float32)
    merged = 0.5 * (fold_values + jnp.take(fold_values, partner, axis=2))

    def per_field(items):
        one_field, merged_row = items
        sums = jnp.sum(one_field.astype(jnp.float32) * weight, axis=-1)
        fold_sum = jnp.sum(merged_row * weight[:, NLAT - 1, :], axis=-1)
        return sums.at[:, NLAT - 1].set(fold_sum)

    row_sum = lax.map(per_field, (fields, merged))
    return row_sum / row_weight[None]
```

```python
import functools

import jax
import jax.numpy as jnp
from jax import lax
from jax.experimental import pallas as pl
from jax.experimental.pallas import tpu as pltpu
from jax.sharding import PartitionSpec as P

MESH = pl.DeviceIdType.MESH
GROUP = 8


def kernel(
    dims, fields, area, ocean, partner, counted, out,
    fv, av, ov, pv, cv, wt, wf, hb, part, recv,
    fsem, isem, hs, hr, ps, pr, zs, zr, x0s, x0r, y1s, y1r, y0s, y0r, x1s, x1r, ws, wr, cs, cr,
):
    n_lat, n_lon, nx, nz, ny, nc = dims
    levels, lat_rows, lon_cols = ocean.shape
    rows = fields.shape[0] // n_lon
    groups = rows // GROUP
    first = (groups + 1) // 2 * GROUP
    band, me = lax.axis_index("lat"), lax.axis_index("lon")
    z, x = band // nx, band % nx
    y, core = me // nc, me % nc
    top = band == n_lat - 1
    targets = [(dy, dc) for dy in range(1, ny) for dc in range(nc)]
    targets += [(0, dc) for dc in range(1, nc)]

    def lon_at(dy, dc):
        return ((y + dy) % ny) * nc + (core + dc) % nc

    def lat_at(dz, dx):
        return ((z + dz) % nz) * nx + (x + dx) % nx

    ins = [
        pltpu.make_async_copy(ocean, ov, isem.at[0]),
        pltpu.make_async_copy(area, av, isem.at[1]),
        pltpu.make_async_copy(partner, pv, isem.at[2]),
        pltpu.make_async_copy(counted, cv, isem.at[3]),
    ]
    for c in ins:
        c.start()

    def load(index):
        at = pl.ds(pl.multiple_of(index * GROUP, GROUP), GROUP)
        return pltpu.make_async_copy(fields.at[at], fv.at[at], fsem.at[index])

    for dy, dc in targets + [(0, 0)]:
        owner = lon_at(dy, dc)

        def begin(g, carry, owner=owner):
            load(owner * groups + g).start()
            return carry

        lax.fori_loop(0, groups, begin, 0)

    barrier = pltpu.get_barrier_semaphore()
    greeted = [(0, 0, dy, dc) for dy, dc in targets]
    greeted += [(dz, 0, 0, 0) for dz in range(1, nz)]
    greeted += [(0, dx, 0, 0) for dx in range(1, nx)]
    for dz, dx, dy, dc in greeted:
        pl.semaphore_signal(
            barrier, inc=1, device_id={"lat": lat_at(dz, dx), "lon": lon_at(dy, dc)}, device_id_type=MESH
        )
    pl.semaphore_wait(barrier, len(greeted))

    for c in ins:
        c.wait()
    own_lanes = pl.ds(pl.multiple_of(me * lon_cols, lon_cols), lon_cols)

    @pl.when(top)
    def _():
        fold_ocean = jnp.concatenate(
            [ov[l, lat_rows - 1 : lat_rows, :] for l in range(levels)], axis=0
        ).astype(jnp.float32)
        fold_cell = cv[:, own_lanes].astype(jnp.float32) * av[lat_rows - 1 : lat_rows, :]
        hb[me] = 0.5 * (fold_cell * fold_ocean)

        def h_copy(k, dy, dc, slot):
            return pltpu.make_async_remote_copy(
                src_ref=hb.at[slot], dst_ref=hb.at[slot], send_sem=hs.at[k], recv_sem=hr.at[k],
                device_id={"lat": band, "lon": lon_at(dy, dc)}, device_id_type=MESH,
            )

        for k, (dy, dc) in enumerate(targets):
            h_copy(k, dy, dc, me).start()
        for k, (dy, dc) in enumerate(targets):
            h_copy(k, dy, dc, lon_at(-dy, -dc)).wait_recv()
        whole = jnp.concatenate([hb[q] for q in range(n_lon)], axis=1)
        columns = lax.broadcasted_iota(jnp.int32, (n_lon * lon_cols, lon_cols), 0)
        chosen = (columns == pv[:, own_lanes]).astype(jnp.float32)
        joined = lax.dot_general(
            whole, chosen, (((1,), (0,)), ((), ())),
            precision=lax.Precision.HIGHEST, preferred_element_type=jnp.float32,
        )
        wf[...] = hb[me] + joined
        for k, (dy, dc) in enumerate(targets):
            h_copy(k, dy, dc, me).wait_send()

    @pl.when(jnp.logical_not(top))
    def _():
        wf[...] = jnp.zeros_like(wf)

    fold = jnp.logical_and(
        lax.broadcasted_iota(jnp.int32, (lat_rows, lon_cols), 0) == lat_rows - 1, top
    )
    cell = jnp.where(fold, cv[:, own_lanes].astype(jnp.float32), 1.0) * av[...]

    def weigh(l, carry):
        sea = ov[l].astype(jnp.float32)
        weight = jnp.where(fold, wf[pl.ds(l, 1), :], cell * sea)
        wt[l] = weight.T
        part[me, pl.ds(rows + l, 1), :] = jnp.sum((cell * (sea + 0.05)).T, axis=0, keepdims=True)
        return carry

    lax.fori_loop(0, levels, weigh, 0)
    for dy, dc in targets:
        part[lon_at(dy, dc), rows:, :] = part[me, rows:, :]

    def p_copy(k, dy, dc, src, dst):
        return pltpu.make_async_remote_copy(
            src_ref=part.at[src], dst_ref=recv.at[dst], send_sem=ps.at[k], recv_sem=pr.at[k],
            device_id={"lat": band, "lon": lon_at(dy, dc)}, device_id_type=MESH,
        )

    for k, (dy, dc) in enumerate(targets + [(0, 0)]):
        owner = lon_at(dy, dc)

        def reduce(g, carry, owner=owner):
            index = owner * groups + g
            load(index).wait()
            base = pl.multiple_of((index * GROUP) % levels, GROUP)
            sums = []
            for r in range(GROUP):
                turned = fv[index * GROUP + r].T.astype(jnp.float32)
                sums.append(jnp.sum(turned * wt[base + r], axis=0, keepdims=True))
            part[owner, pl.ds(pl.multiple_of(g * GROUP, GROUP), GROUP), :] = jnp.concatenate(sums, axis=0)
            return carry

        lax.fori_loop(0, groups, reduce, 0)
        if k < len(targets):
            p_copy(k, dy, dc, owner, me).start()

    for k, (dy, dc) in enumerate(targets):
        p_copy(k, dy, dc, me, lon_at(-dy, -dc)).wait_recv()

    slots = [lon_at(dy, dc) for dy, dc in targets]
    total_weight = part[me, rows:, :]
    for s in slots:
        total_weight += recv[s, rows:, :]
    part[me, rows:, :] = total_weight

    def region(dz, dx, dy, dc, half):
        start, size = ((0, rows), (0, first), (first, rows - first))[half]
        return out.at[
            pl.ds(pl.multiple_of(lon_at(dy, dc) * rows + start, GROUP), size),
            pl.ds(pl.multiple_of(lat_at(dz, dx) * lat_rows, lat_rows), lat_rows),
        ]

    own_band = pl.ds(pl.multiple_of(band * lat_rows, lat_rows), lat_rows)
    for g in range(groups):
        at = slice(g * GROUP, (g + 1) * GROUP)
        total = part[me, at, :]
        for s in slots:
            total += recv[s, at, :]
        index = me * groups + g
        base = pl.multiple_of((index * GROUP) % levels, GROUP)
        out[pl.ds(pl.multiple_of(index * GROUP, GROUP), GROUP), own_band] = (
            total / part[me, pl.ds(rows + base, GROUP), :]
        )

    sent = []

    def move(block, half, send, receive, to):
        c = pltpu.make_async_remote_copy(
            src_ref=region(*block, half), dst_ref=region(*block, half), send_sem=send, recv_sem=receive,
            device_id={"lat": lat_at(to[0], to[1]), "lon": lon_at(to[2], to[3])}, device_id_type=MESH,
        )
        return c

    def send(*a):
        c = move(*a)
        c.start()
        sent.append(c)

    handed = []

    def hand(block, half):
        for dc in range(1, nc):
            k = len(handed)
            send(block, half, cs.at[k], cr.at[k], (0, 0, 0, dc))
            handed.append((block[:3] + (-dc,), half, k, dc))

    order = sorted(range(1, nz), key=lambda d: min(d, nz - d))
    for d in order:
        send((0, 0, 0, 0), 0, zs.at[d], zr.at[d], (d, 0, 0, 0))
    for d in [0] + order:
        block = (-d, 0, 0, 0)
        if d:
            move(block, 0, zs.at[d], zr.at[d], (d, 0, 0, 0)).wait_recv()
        for e in range(1, nx):
            send(block, 0, x0s.at[d, e], x0r.at[d, e], (0, e, 0, 0))
        for e in range(1, ny):
            send(block, 0, y1s.at[d, e], y1r.at[d, e], (0, 0, e, 0))
        hand(block, 0)
    for d in [0] + order:
        for e in range(1, nx):
            block = (-d, -e, 0, 0)
            move(block, 0, x0s.at[d, e], x0r.at[d, e], (0, e, 0, 0)).wait_recv()
            for k in range(1, ny):
                send(block, 1, y0s.at[d, e, k], y0r.at[d, e, k], (0, 0, k, 0))
            hand(block, 0)
        for e in range(1, ny):
            block = (-d, 0, -e, 0)
            move(block, 0, y1s.at[d, e], y1r.at[d, e], (0, 0, e, 0)).wait_recv()
            for k in range(1, nx):
                send(block, 2, x1s.at[d, e, k], x1r.at[d, e, k], (0, k, 0, 0))
            hand(block, 0)
    for d in [0] + order:
        for e in range(1, nx):
            for k in range(1, ny):
                block = (-d, -e, -k, 0)
                move(block, 1, y0s.at[d, e, k], y0r.at[d, e, k], (0, 0, k, 0)).wait_recv()
                hand(block, 1)
        for e in range(1, ny):
            for k in range(1, nx):
                block = (-d, -k, -e, 0)
                move(block, 2, x1s.at[d, e, k], x1r.at[d, e, k], (0, k, 0, 0)).wait_recv()
                hand(block, 2)
    for block, half, k, dc in handed:
        move(block, half, cs.at[k], cr.at[k], (0, 0, 0, dc)).wait_recv()
    for c in sent:
        c.wait_send()
    for k, (dy, dc) in enumerate(targets):
        p_copy(k, dy, dc, lon_at(dy, dc), me).wait_send()


def per_device(dims, fields, area, ocean, partner, counted):
    n_lat, n_lon, nx, nz, ny, nc = dims
    count, levels, lat_rows, lon_cols = fields.shape
    total = count * levels
    rows = total // n_lon
    hands = nz * (1 + (nx - 1) + (ny - 1) + 2 * (nx - 1) * (ny - 1)) * max(nc - 1, 1)
    dma = pltpu.SemaphoreType.DMA
    any_space = pl.BlockSpec(memory_space=pl.ANY)
    zonal = pl.pallas_call(
        functools.partial(kernel, dims),
        out_shape=jax.ShapeDtypeStruct((total, n_lat * lat_rows), jnp.float32),
        in_specs=[any_space] * 5,
        out_specs=pl.BlockSpec(memory_space=pltpu.VMEM),
        scratch_shapes=[
            pltpu.VMEM((total, lat_rows, lon_cols), fields.dtype),
            pltpu.VMEM((lat_rows, lon_cols), jnp.float32),
            pltpu.VMEM((levels, lat_rows, lon_cols), jnp.int32),
            pltpu.VMEM((1, n_lon * lon_cols), jnp.int32),
            pltpu.VMEM((1, n_lon * lon_cols), jnp.int32),
            pltpu.VMEM((levels, lon_cols, lat_rows), jnp.float32),
            pltpu.VMEM((levels, lon_cols), jnp.float32),
            pltpu.VMEM((n_lon, levels, lon_cols), jnp.float32),
            pltpu.VMEM((n_lon, rows + levels, lat_rows), jnp.float32),
            pltpu.VMEM((n_lon, rows + levels, lat_rows), jnp.float32),
            dma((total // GROUP,)),
            dma((4,)),
            dma((n_lon,)), dma((n_lon,)),
            dma((n_lon,)), dma((n_lon,)),
            dma((nz,)), dma((nz,)),
            dma((nz, nx)), dma((nz, nx)),
            dma((nz, ny)), dma((nz, ny)),
            dma((nz, nx, ny)), dma((nz, nx, ny)),
            dma((nz, ny, nx)), dma((nz, ny, nx)),
            dma((1,)), dma((1,)),
            dma((hands,)), dma((hands,)),
        ],
        compiler_params=pltpu.CompilerParams(collective_id=0, has_side_effects=True),
    )(
        fields.reshape(total, lat_rows, lon_cols), area, ocean,
        partner.reshape(1, -1), counted.reshape(1, -1),
    )
    return zonal.reshape(count, levels, n_lat * lat_rows)


def solution(mesh):
    n_lat, n_lon = mesh.shape["lat"], mesh.shape["lon"]
    nc = 2 if n_lon % 2 == 0 else 1
    ny = n_lon // nc
    nx = ny if n_lat % ny == 0 else 1
    dims = (n_lat, n_lon, nx, n_lat // nx, ny, nc)
    in_specs = (P(None, None, "lat", "lon"), P("lat", "lon"), P(None, "lat", "lon"), P(), P())
    return jax.shard_map(
        functools.partial(per_device, dims), mesh=mesh, in_specs=in_specs, out_specs=P(), check_vma=False
    )
```

```python
import functools

import jax
import jax.numpy as jnp
from jax import lax
from jax.experimental import pallas as pl
from jax.experimental.pallas import tpu as pltpu
from jax.sharding import PartitionSpec as P

MESH = pl.DeviceIdType.MESH
GROUP = 8
PACK = 16
TOP_CODE = 32767.0
LEAST = 1e-33


def step_of(exponent):
    return jnp.exp2(exponent) * (1.0 / TOP_CODE)


def kernel(
    dims, fields, area, ocean, partner, counted, out,
    fv, av, ov, pv, cv, wt, hb, part, recv,
    fsem, isem, hs, hr, ps, pr, zs, zr, x0s, x0r, y1s, y1r, y0s, y0r, x1s, x1r, ws, wr, cs, cr,
):
    n_lat, n_lon, nx, nz, ny, nc = dims
    levels, lat_rows, lon_cols = ocean.shape
    rows = fields.shape[0] // n_lon
    groups = rows // GROUP
    coded = out.shape[2]
    first = (coded // PACK + 1) // 2 * PACK
    band, me = lax.axis_index("lat"), lax.axis_index("lon")
    z, x = band // nx, band % nx
    y, core = me // nc, me % nc
    top = band == n_lat - 1
    targets = [(dy, dc) for dy in range(1, ny) for dc in range(nc)]
    targets += [(0, dc) for dc in range(1, nc)]

    def lon_at(dy, dc):
        return ((y + dy) % ny) * nc + (core + dc) % nc

    def lat_at(dz, dx):
        return ((z + dz) % nz) * nx + (x + dx) % nx

    ins = [
        pltpu.make_async_copy(ocean, ov, isem.at[0]),
        pltpu.make_async_copy(area, av, isem.at[1]),
        pltpu.make_async_copy(partner, pv, isem.at[2]),
        pltpu.make_async_copy(counted, cv, isem.at[3]),
    ]
    for c in ins:
        c.start()

    def load(index):
        at = pl.ds(pl.multiple_of(index * GROUP, GROUP), GROUP)
        return pltpu.make_async_copy(fields.at[at], fv.at[at], fsem.at[index])

    for dy, dc in targets + [(0, 0)]:
        owner = lon_at(dy, dc)

        def begin(g, carry, owner=owner):
            load(owner * groups + g).start()
            return carry

        lax.fori_loop(0, groups, begin, 0)

    barrier = pltpu.get_barrier_semaphore()
    greeted = [(0, 0, dy, dc) for dy, dc in targets]
    greeted += [(dz, 0, 0, 0) for dz in range(1, nz)]
    greeted += [(0, dx, 0, 0) for dx in range(1, nx)]
    for dz, dx, dy, dc in greeted:
        pl.semaphore_signal(
            barrier, inc=1, device_id={"lat": lat_at(dz, dx), "lon": lon_at(dy, dc)}, device_id_type=MESH
        )
    for c in ins:
        c.wait()
    own_lanes = pl.ds(pl.multiple_of(me * lon_cols, lon_cols), lon_cols)

    fold = jnp.logical_and(
        lax.broadcasted_iota(jnp.int32, (lat_rows, lon_cols), 0) == lat_rows - 1, top
    )
    cell = (jnp.where(fold, cv[:, own_lanes].astype(jnp.float32), 1.0) * av[...]).T

    def weigh(l, carry):
        sea = ov[l].astype(jnp.float32).T
        wt[l] = cell * sea
        part[me, pl.ds(rows + l, 1), :] = jnp.sum(cell * (sea + 0.05), axis=0, keepdims=True)
        return carry

    lax.fori_loop(0, levels, weigh, 0, unroll=2)
    pl.semaphore_wait(barrier, len(greeted))

    @pl.when(top)
    def _():
        fold_ocean = jnp.concatenate(
            [ov[l, lat_rows - 1 : lat_rows, :] for l in range(levels)], axis=0
        ).astype(jnp.float32)
        fold_cell = cv[:, own_lanes].astype(jnp.float32) * av[lat_rows - 1 : lat_rows, :]
        hb[me] = 0.5 * (fold_cell * fold_ocean)

        def h_copy(k, dy, dc, slot):
            return pltpu.make_async_remote_copy(
                src_ref=hb.at[slot], dst_ref=hb.at[slot], send_sem=hs.at[k], recv_sem=hr.at[k],
                device_id={"lat": band, "lon": lon_at(dy, dc)}, device_id_type=MESH,
            )

        for k, (dy, dc) in enumerate(targets):
            h_copy(k, dy, dc, me).start()
        for k, (dy, dc) in enumerate(targets):
            h_copy(k, dy, dc, lon_at(-dy, -dc)).wait_recv()
        whole = jnp.concatenate([hb[q] for q in range(n_lon)], axis=1)
        columns = lax.broadcasted_iota(jnp.int32, (n_lon * lon_cols, lon_cols), 0)
        chosen = (columns == pv[:, own_lanes]).astype(jnp.float32)
        joined = lax.dot_general(
            whole, chosen, (((1,), (0,)), ((), ())),
            precision=lax.Precision.HIGHEST, preferred_element_type=jnp.float32,
        )
        filler = jnp.zeros((lon_cols - levels, lon_cols), jnp.float32)
        column = jnp.concatenate([hb[me] + joined, filler], axis=0).T
        last = lax.broadcasted_iota(jnp.int32, (lon_cols, lat_rows), 1) == lat_rows - 1
        for l in range(levels):
            wt[l] = jnp.where(last, column[:, l : l + 1], wt[l])
        for k, (dy, dc) in enumerate(targets):
            h_copy(k, dy, dc, me).wait_send()

    for dy, dc in targets:
        part[lon_at(dy, dc), rows:, :] = part[me, rows:, :]

    def p_copy(k, dy, dc, src, dst):
        return pltpu.make_async_remote_copy(
            src_ref=part.at[src], dst_ref=recv.at[dst], send_sem=ps.at[k], recv_sem=pr.at[k],
            device_id={"lat": band, "lon": lon_at(dy, dc)}, device_id_type=MESH,
        )

    for k, (dy, dc) in enumerate(targets + [(0, 0)]):
        owner = lon_at(dy, dc)

        def reduce(g, carry, owner=owner):
            index = owner * groups + g
            load(index).wait()
            base = pl.multiple_of((index * GROUP) % levels, GROUP)
            sums = []
            for r in range(GROUP):
                turned = fv[index * GROUP + r].T.astype(jnp.float32)
                sums.append(jnp.sum(turned * wt[base + r], axis=0, keepdims=True))
            part[owner, pl.ds(pl.multiple_of(g * GROUP, GROUP), GROUP), :] = jnp.concatenate(sums, axis=0)
            return carry

        lax.fori_loop(0, groups, reduce, 0)
        if k < len(targets):
            p_copy(k, dy, dc, owner, me).start()

    for k, (dy, dc) in enumerate(targets):
        p_copy(k, dy, dc, me, lon_at(-dy, -dc)).wait_recv()

    slots = [lon_at(dy, dc) for dy, dc in targets]
    total_weight = part[me, rows:, :]
    for s in slots:
        total_weight += recv[s, rows:, :]
    part[me, rows:, :] = total_weight

    def region(dz, dx, dy, dc, half):
        start, size = ((0, coded), (0, first), (first, coded - first))[half]
        return out.at[lat_at(dz, dx), lon_at(dy, dc), pl.ds(start, size)]

    means = []
    for g in range(groups):
        at = slice(g * GROUP, (g + 1) * GROUP)
        total = part[me, at, :]
        for s in slots:
            total += recv[s, at, :]
        base = pl.multiple_of(((me * groups + g) * GROUP) % levels, GROUP)
        means.append(total / part[me, pl.ds(rows + base, GROUP), :])
    mean = jnp.concatenate(means, axis=0)
    largest = jnp.maximum(jnp.max(jnp.abs(mean), axis=0, keepdims=True), LEAST)
    exponent = jnp.ceil(jnp.log2(largest) + 1e-4)
    codes = jnp.round(mean / step_of(exponent))
    tail = jnp.broadcast_to(exponent, (coded - rows, exponent.shape[1]))
    block = jnp.concatenate([codes, tail], axis=0).astype(jnp.int32)
    out[band, me] = block.astype(jnp.int16)

    sent = []

    def move(block, half, send, receive, to):
        c = pltpu.make_async_remote_copy(
            src_ref=region(*block, half), dst_ref=region(*block, half), send_sem=send, recv_sem=receive,
            device_id={"lat": lat_at(to[0], to[1]), "lon": lon_at(to[2], to[3])}, device_id_type=MESH,
        )
        return c

    def send(*a):
        c = move(*a)
        c.start()
        sent.append(c)

    handed = []

    def hand(block, half):
        for dc in range(1, nc):
            k = len(handed)
            send(block, half, cs.at[k], cr.at[k], (0, 0, 0, dc))
            handed.append((block[:3] + (-dc,), half, k, dc))

    order = sorted(range(1, nz), key=lambda d: min(d, nz - d))
    for d in order:
        send((0, 0, 0, 0), 0, zs.at[d], zr.at[d], (d, 0, 0, 0))
    for d in [0] + order:
        block = (-d, 0, 0, 0)
        if d:
            move(block, 0, zs.at[d], zr.at[d], (d, 0, 0, 0)).wait_recv()
        for e in range(1, nx):
            send(block, 0, x0s.at[d, e], x0r.at[d, e], (0, e, 0, 0))
        for e in range(1, ny):
            send(block, 0, y1s.at[d, e], y1r.at[d, e], (0, 0, e, 0))
        hand(block, 0)
    for d in [0] + order:
        for e in range(1, nx):
            block = (-d, -e, 0, 0)
            move(block, 0, x0s.at[d, e], x0r.at[d, e], (0, e, 0, 0)).wait_recv()
            for k in range(1, ny):
                send(block, 1, y0s.at[d, e, k], y0r.at[d, e, k], (0, 0, k, 0))
            hand(block, 0)
        for e in range(1, ny):
            block = (-d, 0, -e, 0)
            move(block, 0, y1s.at[d, e], y1r.at[d, e], (0, 0, e, 0)).wait_recv()
            for k in range(1, nx):
                send(block, 2, x1s.at[d, e, k], x1r.at[d, e, k], (0, k, 0, 0))
            hand(block, 0)
    for d in [0] + order:
        for e in range(1, nx):
            for k in range(1, ny):
                block = (-d, -e, -k, 0)
                move(block, 1, y0s.at[d, e, k], y0r.at[d, e, k], (0, 0, k, 0)).wait_recv()
                hand(block, 1)
        for e in range(1, ny):
            for k in range(1, nx):
                block = (-d, -k, -e, 0)
                move(block, 2, x1s.at[d, e, k], x1r.at[d, e, k], (0, k, 0, 0)).wait_recv()
                hand(block, 2)
    for block, half, k, dc in handed:
        move(block, half, cs.at[k], cr.at[k], (0, 0, 0, dc)).wait_recv()
    for c in sent:
        c.wait_send()
    for k, (dy, dc) in enumerate(targets):
        p_copy(k, dy, dc, lon_at(dy, dc), me).wait_send()


def decode(codes, out):
    n_lon, rows = codes.shape[1], out.shape[0] // codes.shape[1]
    for q in range(n_lon):
        block = codes[0, q].astype(jnp.int32).astype(jnp.float32)
        out[q * rows : (q + 1) * rows, :] = block[:rows] * step_of(block[rows : rows + 1])


def per_device(dims, fields, area, ocean, partner, counted):
    n_lat, n_lon, nx, nz, ny, nc = dims
    count, levels, lat_rows, lon_cols = fields.shape
    total = count * levels
    rows = total // n_lon
    hands = nz * (1 + (nx - 1) + (ny - 1) + 2 * (nx - 1) * (ny - 1)) * max(nc - 1, 1)
    dma = pltpu.SemaphoreType.DMA
    any_space = pl.BlockSpec(memory_space=pl.ANY)
    coded = (rows + PACK) // PACK * PACK
    codes = pl.pallas_call(
        functools.partial(kernel, dims),
        out_shape=jax.ShapeDtypeStruct((n_lat, n_lon, coded, lat_rows), jnp.int16),
        in_specs=[any_space] * 5,
        out_specs=pl.BlockSpec(memory_space=pltpu.VMEM),
        scratch_shapes=[
            pltpu.VMEM((total, lat_rows, lon_cols), fields.dtype),
            pltpu.VMEM((lat_rows, lon_cols), jnp.float32),
            pltpu.VMEM((levels, lat_rows, lon_cols), jnp.int32),
            pltpu.VMEM((1, n_lon * lon_cols), jnp.int32),
            pltpu.VMEM((1, n_lon * lon_cols), jnp.int32),
            pltpu.VMEM((levels, lon_cols, lat_rows), jnp.float32),
            pltpu.VMEM((n_lon, levels, lon_cols), jnp.float32),
            pltpu.VMEM((n_lon, rows + levels, lat_rows), jnp.float32),
            pltpu.VMEM((n_lon, rows + levels, lat_rows), jnp.float32),
            dma((total // GROUP,)),
            dma((4,)),
            dma((n_lon,)), dma((n_lon,)),
            dma((n_lon,)), dma((n_lon,)),
            dma((nz,)), dma((nz,)),
            dma((nz, nx)), dma((nz, nx)),
            dma((nz, ny)), dma((nz, ny)),
            dma((nz, nx, ny)), dma((nz, nx, ny)),
            dma((nz, ny, nx)), dma((nz, ny, nx)),
            dma((1,)), dma((1,)),
            dma((hands,)), dma((hands,)),
        ],
        compiler_params=pltpu.CompilerParams(collective_id=0, has_side_effects=True),
    )(
        fields.reshape(total, lat_rows, lon_cols), area, ocean,
        partner.reshape(1, -1), counted.reshape(1, -1),
    )
    zonal = pl.pallas_call(
        decode,
        grid=(n_lat,),
        out_shape=jax.ShapeDtypeStruct((total, n_lat * lat_rows), jnp.float32),
        in_specs=[pl.BlockSpec((1, n_lon, coded, lat_rows), lambda b: (b, 0, 0, 0))],
        out_specs=pl.BlockSpec((total, lat_rows), lambda b: (0, b)),
    )(codes)
    return zonal.reshape(count, levels, n_lat * lat_rows)


def solution(mesh):
    n_lat, n_lon = mesh.shape["lat"], mesh.shape["lon"]
    nc = 2 if n_lon % 2 == 0 else 1
    ny = n_lon // nc
    nx = ny if n_lat % ny == 0 else 1
    dims = (n_lat, n_lon, nx, n_lat // nx, ny, nc)
    in_specs = (P(None, None, "lat", "lon"), P("lat", "lon"), P(None, "lat", "lon"), P(), P())
    return jax.shard_map(
        functools.partial(per_device, dims), mesh=mesh, in_specs=in_specs, out_specs=P(), check_vma=False
    )
```

```python
import functools

import jax
import jax.numpy as jnp
from jax import lax
from jax.experimental import pallas as pl
from jax.experimental.pallas import tpu as pltpu
from jax.sharding import PartitionSpec as P

MESH = pl.DeviceIdType.MESH
GROUP = 8
PACK = 16
TOP_CODE = 32767.0
LEAST = 1e-33


def step_of(exponent):
    return jnp.exp2(exponent) * (1.0 / TOP_CODE)


def kernel(
    dims, fields, area, ocean, partner, counted, out,
    fv, av, ov, pv, cv, wt, hb, part, recv,
    fsem, isem, hs, hr, ps, pr, zs, zr, x0s, x0r, y1s, y1r, y0s, y0r, x1s, x1r, ws, wr, cs, cr,
):
    n_lat, n_lon, nx, nz, ny, nc = dims
    levels, lat_rows, lon_cols = ocean.shape
    rows = fields.shape[0] // n_lon
    groups = rows // GROUP
    coded = out.shape[2]
    first = (coded // PACK + 1) // 2 * PACK
    band, me = lax.axis_index("lat"), lax.axis_index("lon")
    z, x = band // nx, band % nx
    y, core = me // nc, me % nc
    top = band == n_lat - 1
    targets = [(dy, dc) for dy in range(1, ny) for dc in range(nc)]
    targets += [(0, dc) for dc in range(1, nc)]

    def lon_at(dy, dc):
        return ((y + dy) % ny) * nc + (core + dc) % nc

    def lat_at(dz, dx):
        return ((z + dz) % nz) * nx + (x + dx) % nx

    ins = [
        pltpu.make_async_copy(ocean, ov, isem.at[0]),
        pltpu.make_async_copy(area, av, isem.at[1]),
        pltpu.make_async_copy(partner, pv, isem.at[2]),
        pltpu.make_async_copy(counted, cv, isem.at[3]),
    ]
    for c in ins:
        c.start()

    def load(index):
        at = pl.ds(pl.multiple_of(index * GROUP, GROUP), GROUP)
        return pltpu.make_async_copy(fields.at[at], fv.at[at], fsem.at[index])

    for dy, dc in targets + [(0, 0)]:
        owner = lon_at(dy, dc)

        def begin(g, carry, owner=owner):
            load(owner * groups + g).start()
            return carry

        lax.fori_loop(0, groups, begin, 0)

    barrier = pltpu.get_barrier_semaphore()
    greeted = [(0, 0, dy, dc) for dy, dc in targets]
    greeted += [(dz, 0, 0, 0) for dz in range(1, nz)]
    greeted += [(0, dx, 0, 0) for dx in range(1, nx)]
    for dz, dx, dy, dc in greeted:
        pl.semaphore_signal(
            barrier, inc=1, device_id={"lat": lat_at(dz, dx), "lon": lon_at(dy, dc)}, device_id_type=MESH
        )
    for c in ins:
        c.wait()
    own_lanes = pl.ds(pl.multiple_of(me * lon_cols, lon_cols), lon_cols)

    fold = jnp.logical_and(
        lax.broadcasted_iota(jnp.int32, (lat_rows, lon_cols), 0) == lat_rows - 1, top
    )
    cell = (jnp.where(fold, cv[:, own_lanes].astype(jnp.float32), 1.0) * av[...]).T

    def weigh(l, carry):
        sea = ov[l].astype(jnp.float32).T
        wt[l] = cell * sea
        part[me, pl.ds(rows + l, 1), :] = jnp.sum(cell * (sea + 0.05), axis=0, keepdims=True)
        return carry

    lax.fori_loop(0, levels, weigh, 0, unroll=2)
    pl.semaphore_wait(barrier, len(greeted))

    @pl.when(top)
    def _():
        fold_ocean = jnp.concatenate(
            [ov[l, lat_rows - 1 : lat_rows, :] for l in range(levels)], axis=0
        ).astype(jnp.float32)
        fold_cell = cv[:, own_lanes].astype(jnp.float32) * av[lat_rows - 1 : lat_rows, :]
        hb[me] = 0.5 * (fold_cell * fold_ocean)

        def h_copy(k, dy, dc, slot):
            return pltpu.make_async_remote_copy(
                src_ref=hb.at[slot], dst_ref=hb.at[slot], send_sem=hs.at[k], recv_sem=hr.at[k],
                device_id={"lat": band, "lon": lon_at(dy, dc)}, device_id_type=MESH,
            )

        for k, (dy, dc) in enumerate(targets):
            h_copy(k, dy, dc, me).start()
        for k, (dy, dc) in enumerate(targets):
            h_copy(k, dy, dc, lon_at(-dy, -dc)).wait_recv()
        whole = jnp.concatenate([hb[q] for q in range(n_lon)], axis=1)
        columns = lax.broadcasted_iota(jnp.int32, (n_lon * lon_cols, lon_cols), 0)
        chosen = (columns == pv[:, own_lanes]).astype(jnp.float32)
        joined = lax.dot_general(
            whole, chosen, (((1,), (0,)), ((), ())),
            precision=lax.Precision.HIGHEST, preferred_element_type=jnp.float32,
        )
        filler = jnp.zeros((lon_cols - levels, lon_cols), jnp.float32)
        column = jnp.concatenate([hb[me] + joined, filler], axis=0).T
        last = lax.broadcasted_iota(jnp.int32, (lon_cols, lat_rows), 1) == lat_rows - 1
        for l in range(levels):
            wt[l] = jnp.where(last, column[:, l : l + 1], wt[l])
        for k, (dy, dc) in enumerate(targets):
            h_copy(k, dy, dc, me).wait_send()

    for dy, dc in targets:
        part[lon_at(dy, dc), rows:, :] = part[me, rows:, :]

    def p_copy(k, dy, dc, src, dst):
        return pltpu.make_async_remote_copy(
            src_ref=part.at[src], dst_ref=recv.at[dst], send_sem=ps.at[k], recv_sem=pr.at[k],
            device_id={"lat": band, "lon": lon_at(dy, dc)}, device_id_type=MESH,
        )

    for k, (dy, dc) in enumerate(targets + [(0, 0)]):
        owner = lon_at(dy, dc)

        def reduce(g, carry, owner=owner):
            index = owner * groups + g
            load(index).wait()
            base = pl.multiple_of((index * GROUP) % levels, GROUP)
            sums = []
            for r in range(GROUP):
                turned = fv[index * GROUP + r].T.astype(jnp.float32)
                sums.append(jnp.sum(turned * wt[base + r], axis=0, keepdims=True))
            part[owner, pl.ds(pl.multiple_of(g * GROUP, GROUP), GROUP), :] = jnp.concatenate(sums, axis=0)
            return carry

        lax.fori_loop(0, groups, reduce, 0)
        if k < len(targets):
            p_copy(k, dy, dc, owner, me).start()

    for k, (dy, dc) in enumerate(targets):
        p_copy(k, dy, dc, me, lon_at(-dy, -dc)).wait_recv()

    slots = [lon_at(dy, dc) for dy, dc in targets]
    total_weight = part[me, rows:, :]
    for s in slots:
        total_weight += recv[s, rows:, :]
    part[me, rows:, :] = total_weight

    def region(dz, dx, dy, dc, half):
        start, size = ((0, coded), (0, first), (first, coded - first))[half]
        return out.at[lat_at(dz, dx), lon_at(dy, dc), pl.ds(start, size)]

    means = []
    for g in range(groups):
        at = slice(g * GROUP, (g + 1) * GROUP)
        total = part[me, at, :]
        for s in slots:
            total += recv[s, at, :]
        base = pl.multiple_of(((me * groups + g) * GROUP) % levels, GROUP)
        means.append(total / part[me, pl.ds(rows + base, GROUP), :])
    mean = jnp.concatenate(means, axis=0)
    largest = jnp.maximum(jnp.max(jnp.abs(mean), axis=0, keepdims=True), LEAST)
    exponent = jnp.ceil(jnp.log2(largest) + 1e-4)
    codes = jnp.round(mean / step_of(exponent))
    tail = jnp.broadcast_to(exponent, (coded - rows, exponent.shape[1]))
    block = jnp.concatenate([codes, tail], axis=0).astype(jnp.int32)
    out[band, me] = block.astype(jnp.int16)

    sent = []

    def move(block, half, send, receive, to):
        c = pltpu.make_async_remote_copy(
            src_ref=region(*block, half), dst_ref=region(*block, half), send_sem=send, recv_sem=receive,
            device_id={"lat": lat_at(to[0], to[1]), "lon": lon_at(to[2], to[3])}, device_id_type=MESH,
        )
        return c

    def send(*a):
        c = move(*a)
        c.start()
        sent.append(c)

    handed = []

    def hand(block, half):
        for dc in range(1, nc):
            k = len(handed)
            send(block, half, cs.at[k], cr.at[k], (0, 0, 0, dc))
            handed.append((block[:3] + (-dc,), half, k, dc))

    order = sorted(range(1, nz), key=lambda d: min(d, nz - d))
    for d in order:
        send((0, 0, 0, 0), 0, zs.at[d], zr.at[d], (d, 0, 0, 0))
    for d in [0] + order:
        block = (-d, 0, 0, 0)
        if d:
            move(block, 0, zs.at[d], zr.at[d], (d, 0, 0, 0)).wait_recv()
        for e in range(1, nx):
            send(block, 0, x0s.at[d, e], x0r.at[d, e], (0, e, 0, 0))
        for e in range(1, ny):
            send(block, 0, y1s.at[d, e], y1r.at[d, e], (0, 0, e, 0))
        hand(block, 0)
    for d in [0] + order:
        for e in range(1, nx):
            block = (-d, -e, 0, 0)
            move(block, 0, x0s.at[d, e], x0r.at[d, e], (0, e, 0, 0)).wait_recv()
            for k in range(1, ny):
                send(block, 1, y0s.at[d, e, k], y0r.at[d, e, k], (0, 0, k, 0))
            hand(block, 0)
        for e in range(1, ny):
            block = (-d, 0, -e, 0)
            move(block, 0, y1s.at[d, e], y1r.at[d, e], (0, 0, e, 0)).wait_recv()
            for k in range(1, nx):
                send(block, 2, x1s.at[d, e, k], x1r.at[d, e, k], (0, k, 0, 0))
            hand(block, 0)
    for d in [0] + order:
        for e in range(1, nx):
            for k in range(1, ny):
                block = (-d, -e, -k, 0)
                move(block, 1, y0s.at[d, e, k], y0r.at[d, e, k], (0, 0, k, 0)).wait_recv()
                hand(block, 1)
        for e in range(1, ny):
            for k in range(1, nx):
                block = (-d, -k, -e, 0)
                move(block, 2, x1s.at[d, e, k], x1r.at[d, e, k], (0, k, 0, 0)).wait_recv()
                hand(block, 2)
    for block, half, k, dc in handed:
        move(block, half, cs.at[k], cr.at[k], (0, 0, 0, dc)).wait_recv()
    for c in sent:
        c.wait_send()
    for k, (dy, dc) in enumerate(targets):
        p_copy(k, dy, dc, lon_at(dy, dc), me).wait_send()


def decode(codes, out):
    n_lat, n_lon, coded, lat_rows = codes.shape
    rows = out.shape[0] // n_lon
    for b in range(n_lat):
        for q in range(n_lon):
            block = codes[b, q].astype(jnp.int32).astype(jnp.float32)
            out[q * rows : (q + 1) * rows, b * lat_rows : (b + 1) * lat_rows] = (
                block[:rows] * step_of(block[rows : rows + 1])
            )


def per_device(dims, fields, area, ocean, partner, counted):
    n_lat, n_lon, nx, nz, ny, nc = dims
    count, levels, lat_rows, lon_cols = fields.shape
    total = count * levels
    rows = total // n_lon
    hands = nz * (1 + (nx - 1) + (ny - 1) + 2 * (nx - 1) * (ny - 1)) * max(nc - 1, 1)
    dma = pltpu.SemaphoreType.DMA
    any_space = pl.BlockSpec(memory_space=pl.ANY)
    coded = (rows + PACK) // PACK * PACK
    codes = pl.pallas_call(
        functools.partial(kernel, dims),
        out_shape=jax.ShapeDtypeStruct((n_lat, n_lon, coded, lat_rows), jnp.int16),
        in_specs=[any_space] * 5,
        out_specs=pl.BlockSpec(memory_space=pltpu.VMEM),
        scratch_shapes=[
            pltpu.VMEM((total, lat_rows, lon_cols), fields.dtype),
            pltpu.VMEM((lat_rows, lon_cols), jnp.float32),
            pltpu.VMEM((levels, lat_rows, lon_cols), jnp.int32),
            pltpu.VMEM((1, n_lon * lon_cols), jnp.int32),
            pltpu.VMEM((1, n_lon * lon_cols), jnp.int32),
            pltpu.VMEM((levels, lon_cols, lat_rows), jnp.float32),
            pltpu.VMEM((n_lon, levels, lon_cols), jnp.float32),
            pltpu.VMEM((n_lon, rows + levels, lat_rows), jnp.float32),
            pltpu.VMEM((n_lon, rows + levels, lat_rows), jnp.float32),
            dma((total // GROUP,)),
            dma((4,)),
            dma((n_lon,)), dma((n_lon,)),
            dma((n_lon,)), dma((n_lon,)),
            dma((nz,)), dma((nz,)),
            dma((nz, nx)), dma((nz, nx)),
            dma((nz, ny)), dma((nz, ny)),
            dma((nz, nx, ny)), dma((nz, nx, ny)),
            dma((nz, ny, nx)), dma((nz, ny, nx)),
            dma((1,)), dma((1,)),
            dma((hands,)), dma((hands,)),
        ],
        compiler_params=pltpu.CompilerParams(collective_id=0, has_side_effects=True),
    )(
        fields.reshape(total, lat_rows, lon_cols), area, ocean,
        partner.reshape(1, -1), counted.reshape(1, -1),
    )
    zonal = pl.pallas_call(
        decode,
        out_shape=jax.ShapeDtypeStruct((total, n_lat * lat_rows), jnp.float32),
        in_specs=[pl.BlockSpec(memory_space=pltpu.VMEM)],
        out_specs=pl.BlockSpec(memory_space=pltpu.VMEM),
    )(codes)
    return zonal.reshape(count, levels, n_lat * lat_rows)


def solution(mesh):
    n_lat, n_lon = mesh.shape["lat"], mesh.shape["lon"]
    nc = 2 if n_lon % 2 == 0 else 1
    ny = n_lon // nc
    nx = ny if n_lat % ny == 0 else 1
    dims = (n_lat, n_lon, nx, n_lat // nx, ny, nc)
    in_specs = (P(None, None, "lat", "lon"), P("lat", "lon"), P(None, "lat", "lon"), P(), P())
    return jax.shard_map(
        functools.partial(per_device, dims), mesh=mesh, in_specs=in_specs, out_specs=P(), check_vma=False
    )
```
